32 devices in a mesh: rep: 1, dp: 32 (over x, y, z, core).
Axes of the slice: x: 2, y: 2, z: 4, core: 2. Of those that a mesh axis runs over, the one named last changes fastest.
Arguments:
- x: bfloat16 [32, 2048, 640], P(('rep', 'dp'))
- dy: bfloat16 [32, 2048, 640], P(('rep', 'dp'))
- w_gate: bfloat16 [2, 640, 2048], P(None, 'dp')
- w_up: bfloat16 [2, 640, 2048], P(None, 'dp')
- w_down: bfloat16 [2, 2048, 640], P(None, 'dp')
Outputs:
- output 1: bfloat16 [32, 2048, 640], P(('rep', 'dp'))
- output 2: bfloat16 [2, 640, 2048], P('rep', 'dp')
- output 3: bfloat16 [2, 640, 2048], P('rep', 'dp')
- output 4: bfloat16 [2, 2048, 640], P('rep', 'dp')
All inputs are finite; a program needn't handle non-finite values.
Results may differ from the reference program's by a relative error of at most 0.018.
Values are sent between devices in bfloat16 or wider.
A program may use at most 2 GiB of HBM per device.

```python
import jax
import jax.numpy as jnp
from jax import lax

SEQUENCES = 32
TOKENS = 2048
D = 640
FF = 2048
LAYERS = 2
NAMES = ("w_gate", "w_up", "w_down")
SHAPES = {"w_gate": (LAYERS, D, FF), "w_up": (LAYERS, D, FF), "w_down": (LAYERS, FF, D)}


def bump(key, n, height):
    away = (jnp.arange(n, dtype=jnp.int32) - jax.random.randint(key, (), 0, n, jnp.int32)) % n
    return jnp.where(away < n // 8, height, 1.0)


def together(key, own, strength):
    shared = jax.random.normal(key, own.shape[1:], jnp.float32)
    return (own + strength * shared) * lax.rsqrt(1 + strength * strength)


def setup_inputs(seed: int = 0, part: int = 0) -> dict:
    kx, kdy, ka, kb, kz, kf, kh, kl, *kw = jax.random.split(jax.random.key(seed), 8 + len(NAMES))
    kx, kdy, ka, kb = (jax.random.fold_in(k, part) for k in (kx, kdy, ka, kb))
    shape = (SEQUENCES, TOKENS, D)
    much_x, much_dy = jax.random.uniform(kz, (2,), jnp.float32, 0.0, 1.0)
    layers = 2.0 ** jax.random.uniform(kl, (LAYERS, 1, 1), jnp.float32, -1.0, 1.0)
    x = together(ka, jax.random.normal(kx, shape, jnp.float32), much_x) * bump(kf, D, 4.0)
    dy = together(kb, jax.random.normal(kdy, shape, jnp.float32), much_dy)
    drawn = {"x": x.astype(jnp.bfloat16), "dy": (dy * (SEQUENCES * TOKENS) ** -0.5).astype(jnp.bfloat16)}
    for key, name in zip(kw, NAMES, strict=True):
        w = jax.random.normal(key, SHAPES[name], jnp.float32) * SHAPES[name][1] ** -0.5
        drawn[name] = (w * {"w_gate": 1.0, "w_up": bump(kh, FF, 4.0), "w_down": layers}[name]).astype(jnp.bfloat16)
    return drawn


def matmul(a, w):
    return jnp.dot(a, w, preferred_element_type=jnp.float32).astype(jnp.bfloat16)


def normed(h):
    wide = h.astype(jnp.float32)
    scale = lax.rsqrt(jnp.mean(wide**2, -1, keepdims=True) + 1e-6)
    return (wide * scale).astype(jnp.bfloat16)


def layer(h, w):
    a = normed(h)
    gate = jnp.dot(a, w["w_gate"], preferred_element_type=jnp.float32)
    up = jnp.dot(a, w["w_up"], preferred_element_type=jnp.float32)
    return h + matmul((jax.nn.silu(gate) * up).astype(jnp.bfloat16), w["w_down"])


def stack(weights, h):
    return lax.scan(lambda h, w: (layer(h, w), None), h, weights)[0]


def reference(x, dy, w_gate, w_up, w_down):
    weights = dict(zip(NAMES, (w_gate, w_up, w_down), strict=True))

    def take(so_far, sequence):
        h, by_y = sequence
        _, back = jax.vjp(stack, weights, h)
        by_weights, by_h = back(by_y)
        return jax.tree.map(lambda total, term: total + term.astype(jnp.float32), so_far, by_weights), by_h

    none_yet = {name: jnp.zeros(w.shape, jnp.float32) for name, w in weights.items()}
    by_weights, by_x = lax.scan(take, none_yet, (x, dy))
    return (by_x, *(by_weights[name].astype(jnp.bfloat16) for name in NAMES))
```

```python
import jax
import jax.numpy as jnp
from jax import lax
from jax.sharding import PartitionSpec as P

LAYERS, D, FF = 2, 640, 2048
F32, BF16 = jnp.float32, jnp.bfloat16


def dot(a, b, ca, cb):
    return lax.dot_general(a, b, (((ca,), (cb,)), ((), ())), preferred_element_type=F32)


def solution(mesh):
    n = mesh.shape["dp"]

    def gather(g, u, d):
        flat = jnp.concatenate([t.reshape(-1, 128) for t in (g, u, d)], 0)
        full = lax.all_gather(flat, "dp", axis=0, tiled=False)
        k = g.size // 128
        return (
            full[:, :k].reshape(D, FF),
            full[:, k : 2 * k].reshape(D, FF),
            full[:, 2 * k :].reshape(FF, D),
        )

    def scatter(g, u, d):
        flat = jnp.concatenate([t.reshape(n, -1, 128) for t in (g, u, d)], 1)
        mine = lax.psum_scatter(flat, "dp", scatter_dimension=0, tiled=False)
        k = D * FF // n // 128
        return (
            mine[:k].reshape(D // n, FF),
            mine[k : 2 * k].reshape(D // n, FF),
            mine[2 * k :].reshape(FF // n, D),
        )

    def norm(h):
        wide = h.astype(F32)
        scale = lax.rsqrt(jnp.mean(wide**2, -1, keepdims=True) + 1e-6)
        return wide, scale, (wide * scale).astype(BF16)

    def up_half(a, w):
        gate, up = dot(a, w[0], 1, 0), dot(a, w[1], 1, 0)
        s = jax.nn.sigmoid(gate)
        return gate, up, s, (gate * s * up).astype(BF16)

    def back(dh, wide, scale, a, gate, up, s, p, w):
        dp = dot(dh, w[2], 1, 1).astype(BF16).astype(F32)
        dwd = dot(p, dh, 0, 0).astype(BF16)
        dup = (dp * gate * s).astype(BF16)
        dgate = (dp * up * s * (1 + gate * (1 - s))).astype(BF16)
        dwg = dot(a, dgate, 0, 0).astype(BF16)
        dwu = dot(a, dup, 0, 0).astype(BF16)
        da = dot(dgate, w[0], 1, 1).astype(BF16) + dot(dup, w[1], 1, 1).astype(BF16)
        da = da.astype(F32)
        inner = jnp.mean(da * wide, -1, keepdims=True)
        dwide = scale * da - wide * (scale**3 * inner)
        return (dwg, dwu, dwd), dh + dwide.astype(BF16)

    def body(x, dy, wg, wu, wd):
        x, dy = x[0], dy[0]
        w0 = gather(wg[0], wu[0], wd[0])
        w1 = gather(wg[1], wu[1], wd[1])
        n0 = norm(x)
        g0 = up_half(n0[2], w0)
        h = x + dot(g0[3], w0[2], 1, 0).astype(BF16)
        n1 = norm(h)
        g1 = up_half(n1[2], w1)
        dw1, dh = back(dy, *n1, *g1, w1)
        r1 = scatter(*dw1)
        dw0, dx = back(dh, *n0, *g0, w0)
        r0 = scatter(*dw0)
        return (dx[None], *(jnp.stack([a, b]) for a, b in zip(r0, r1)))

    s = P(("rep", "dp"), None, None)
    ws = P(None, "dp", None)
    return jax.shard_map(
        body, mesh=mesh, in_specs=(s, s, ws, ws, ws), out_specs=(s, *([P("rep", "dp", None)] * 3)), check_vma=False
    )
```
